32 devices in a mesh: group: 8 (over y, x, core), pos: 4 (over z).
Axes of the slice: x: 2, y: 2, z: 4, core: 2. Of those that a mesh axis runs over, the one named last changes fastest.
Arguments:
- features: bfloat16 [384, 256, 256], P(('group', 'pos')), may hold values from -6 to 6
- gain_attn: float32 [256], replicated, may hold values from 0.1 to 1.9
- w_query: bfloat16 [256, 256], replicated, as said below
- w_key: bfloat16 [256, 256], replicated, as said below
- w_value: bfloat16 [256, 256], replicated, may hold values from -0.375 to 0.375
- w_out: bfloat16 [256, 256], replicated, may hold values from -0.375 to 0.375
- gain_ffn: float32 [256], replicated, may hold values from 0.1 to 1.9
- w_up: bfloat16 [256, 1024], replicated, may hold values from -0.375 to 0.375
- w_down: bfloat16 [1024, 256], replicated, may hold values from -0.1875 to 0.1875
- counts: int32 [6], replicated, may hold values from 4 to 64, as said below
- offsets: int32 [6], replicated, may hold values from 0 to 380, as said below
Outputs:
- result: bfloat16 [384, 256, 256], P(('group', 'pos'))
The draws below stay inside these ranges and needn't reach their ends.
Inputs may be any that keep to these rules, and one draw needn't show every extreme that they name: `counts`: each mixture has 4 to 64 groups, and one mixture has exactly 64. Mixture m occupies slots offsets[m] to offsets[m] + counts[m] - 1; the mixtures follow one another in order without intersection. `w_query`: a dense matrix of independent entries. `w_key`: a dense matrix of independent entries.
All inputs are finite; a program needn't handle non-finite values.
Results may differ from the reference program's by a relative error of at most 0.0065.
Values may be sent and summed in bfloat16 or wider, within the bound.
No kernel may reach another device: no remote copies, remote signals or barrier semaphores. Data moves between devices by JAX's collectives and lax.ppermute only.
A program may use at most 192 MiB of HBM per device.

```python
import math
import jax
import jax.numpy as jnp
from jax import lax

D = 256
HEADS = 8
FF = 1024
K = 256
MIX = 6
NCH = 384
MAXC = 64
MINC = 4


def group_layout(key):
    base = jax.random.fold_in(key, 31)
    first, second, third = jax.random.split(base, 3)
    counts = jax.random.randint(first, (MIX,), MINC, MAXC + 1, dtype=jnp.int32)
    chosen = jax.random.randint(second, (), 0, MIX, dtype=jnp.int32)
    counts = jnp.where(jnp.arange(MIX, dtype=jnp.int32) == chosen, MAXC, counts).astype(jnp.int32)
    spare = NCH - jnp.sum(counts)
    shares = jax.random.randint(third, (MIX + 1,), 1, 100, dtype=jnp.int32)
    gaps = spare * shares // jnp.sum(shares)
    offsets = jnp.cumsum(gaps[:MIX]) + jnp.cumsum(counts) - counts
    return (counts.astype(jnp.int32), offsets.astype(jnp.int32))


def draw_counts(key, part):
    return group_layout(key)[0]


def draw_offsets(key, part):
    return group_layout(key)[1]


def paired_normals(key):
    shared = jax.random.normal(jax.random.fold_in(key, 41), (D, D), jnp.float32)
    other = jax.random.normal(jax.random.fold_in(key, 43), (D, D), jnp.float32)
    return (shared, other)


def draw_w_query(key, part):
    shared, other = paired_normals(key)
    return (shared / D ** 0.5).astype(jnp.bfloat16)


def draw_w_key(key, part):
    shared, other = paired_normals(key)
    return (other / D ** 0.5).astype(jnp.bfloat16)


def shard_levels(rng, dims, cuts, smallest, high):
    level, own = 1.0, jax.random.fold_in(rng, 6)
    for dim, parts in cuts:
        draws = jnp.exp(jax.random.uniform(jax.random.fold_in(own, dim), (parts,), jnp.float32, smallest / len(cuts), high / len(cuts)))
        level = level * jnp.repeat(draws, dims[dim] // parts).reshape([-1 if axis == dim else 1 for axis in range(len(dims))])
    return level


def gaussian(stream_key, shape, scale, most, shards=(), kind=jnp.bfloat16):
    array = jax.random.normal(stream_key, shape, jnp.float32) * scale
    if len(shards) > 0:
        array = shard_levels(stream_key, shape, shards, -0.22, 0.18) * array
    return jnp.clip(array, min=-most, max=most).astype(kind)


def setup_inputs(seed: int = 0) -> dict:
    seeds = jax.random.split(jax.random.key(seed), 12)
    return {
        "features": gaussian(seeds[0], (NCH, K, D), 1.0, 6.0, ((0, 32),)),
        "gain_attn": jnp.clip(1.0 + 0.18 * jax.random.normal(seeds[1], (D,), jnp.float32), 0.1, 1.9),
        "w_query": draw_w_query(jax.random.fold_in(seeds[11], 71), 0),
        "w_key": draw_w_key(jax.random.fold_in(seeds[11], 71), 0),
        "w_value": gaussian(seeds[4], (D, D), D ** -0.5, 0.375),
        "w_out": gaussian(seeds[5], (D, D), D ** -0.5, 0.375),
        "gain_ffn": jnp.clip(1.0 + 0.18 * jax.random.normal(seeds[6], (D,), jnp.float32), 0.1, 1.9),
        "w_up": gaussian(seeds[7], (D, FF), D ** -0.5, 0.375),
        "w_down": gaussian(seeds[8], (FF, D), FF ** -0.5, 0.1875),
        "counts": draw_counts(jax.random.fold_in(seeds[11], 71), 0),
        "offsets": draw_offsets(jax.random.fold_in(seeds[11], 71), 0),
    }


epsilon = 1e-05
masked_value = -1e+30

def segment_ids(counts, offsets, slots_total):
    slots = jnp.arange(slots_total, dtype=jnp.int32)[:, None]
    inside = (slots >= offsets[None, :]) & (slots < offsets[None, :] + counts[None, :])
    labels = jnp.arange(counts.shape[0], dtype=jnp.int32)[None, :] + 1
    return lax.optimization_barrier(jnp.sum(jnp.where(inside, labels, 0), axis=1)).astype(jnp.int32) - 1

def layer_norm(values, gain):
    floats = values.astype(jnp.float32)
    average = lax.optimization_barrier(jnp.mean(floats, axis=-1, keepdims=True))
    centred = floats - average
    spread = lax.optimization_barrier(jnp.mean(centred * centred, axis=-1, keepdims=True))
    return (centred * lax.rsqrt(spread + epsilon) * gain.astype(jnp.float32)).astype(jnp.bfloat16)

def feed_forward(middle, gain_ffn, w_up, w_down):
    second = layer_norm(middle, gain_ffn)
    hidden = jnp.maximum(jnp.dot(second, w_up, preferred_element_type=jnp.float32), 0.0).astype(jnp.bfloat16)
    return (middle.astype(jnp.float32) + jnp.dot(hidden, w_down, preferred_element_type=jnp.float32)).astype(jnp.bfloat16)

def reference(features, gain_attn, w_query, w_key, w_value, w_out, gain_ffn, w_up, w_down, counts, offsets):
    labels = segment_ids(counts, offsets, NCH)
    living = labels >= 0
    allowed = (labels[:, None] == labels[None, :]) & living[:, None]
    head_dim = D // HEADS
    scale = 1.0 / math.sqrt(head_dim)

    def one_position(column):
        normed = layer_norm(column, gain_attn)
        query = jnp.dot(normed, w_query, preferred_element_type=jnp.float32).astype(jnp.bfloat16).reshape(NCH, HEADS, head_dim)
        keys = jnp.dot(normed, w_key, preferred_element_type=jnp.float32).astype(jnp.bfloat16).reshape(NCH, HEADS, head_dim)
        values = jnp.dot(normed, w_value, preferred_element_type=jnp.float32).astype(jnp.bfloat16).reshape(NCH, HEADS, head_dim)
        scores = jnp.einsum('qhe,khe->hqk', query.astype(jnp.float32), keys.astype(jnp.float32)) * scale
        scores = jnp.where(allowed[None], scores, masked_value)
        highest = lax.optimization_barrier(jnp.max(scores, axis=-1, keepdims=True))
        exponent = jnp.exp(scores - highest)
        total = lax.optimization_barrier(jnp.sum(exponent, axis=-1, keepdims=True))
        weights = (exponent / total).astype(jnp.bfloat16)
        context = jnp.einsum('hqk,khe->qhe', weights.astype(jnp.float32), values.astype(jnp.float32)).astype(jnp.bfloat16).reshape(NCH, D)
        context = jnp.where(living[:, None], context, jnp.zeros_like(context))
        middle = (column.astype(jnp.float32) + jnp.dot(context, w_out, preferred_element_type=jnp.float32)).astype(jnp.bfloat16)
        return feed_forward(middle, gain_ffn, w_up, w_down)
    outputs = lax.map(one_position, jnp.swapaxes(features, 0, 1))
    return jnp.swapaxes(outputs, 0, 1)
```

```python
import functools
import math

import jax
import jax.numpy as jnp
from jax import lax
from jax.experimental import pallas as pl
from jax.experimental.pallas import tpu as pltpu
from jax.sharding import PartitionSpec as P

HEADS = 8
LANES = 128


epsilon = 1e-05
masked_value = -1e30
f32 = jnp.float32
bf16 = jnp.bfloat16


def layer_norm(floats, gain):
    average = jnp.mean(floats, axis=-1, keepdims=True)
    centred = floats - average
    spread = jnp.mean(centred * centred, axis=-1, keepdims=True)
    return (centred * lax.rsqrt(spread + epsilon) * gain).astype(bf16)


def dot(a, b):
    return lax.dot_general(a, b, (((1,), (0,)), ((), ())), preferred_element_type=f32)


def dot_t(a, b):
    return lax.dot_general(a, b, (((1,), (1,)), ((), ())), preferred_element_type=f32)


def iota(shape, dim):
    return lax.broadcasted_iota(jnp.int32, shape, dim)


def attention_kernel(
    window,
    counts_ref,
    offsets_ref,
    x_ref,
    gain_ref,
    wq_ref,
    wk_ref,
    wv_ref,
    wo_ref,
    out_ref,
    q_ref,
    k_ref,
    v_ref,
    c_ref,
):
    slots, owned, width = x_ref.shape
    head_dim = width // HEADS
    mixtures = counts_ref.shape[0]
    span = min(window, max(1, 256 // owned))
    rows = span * owned
    chunks = window // span
    scale = math.log2(math.e) / math.sqrt(head_dim)
    across = max(1, min(HEADS, width // window))
    down = HEADS // across
    row, col = iota((rows, rows), 0), iota((rows, rows), 1)
    to_pos = ((row % span) * owned + row // span == col).astype(f32).astype(bf16)
    to_slot = ((col % span) * owned + col // span == row).astype(f32).astype(bf16)
    gain = gain_ref[...]
    lane = iota((window, width), 1) // head_dim
    in_down = [lane % down == j for j in range(down)]
    in_across = [lane // down == i for i in range(across)]
    key_at = iota((down * window, across * window), 1) % window
    slot_at = iota((rows, width), 0) // owned
    ones = (
        iota((across * window, width), 0) // window
        == iota((across * window, width), 1) // (head_dim * down)
    )
    ones = ones.astype(f32).astype(bf16)
    out_ref[...] = x_ref[...]

    def mixture(m, carry):
        begin, count = offsets_ref[m], counts_ref[m]
        start = jnp.minimum(begin, slots - window)
        low = begin - start
        high = low + count

        def taken(ref, c):
            return ref[pl.ds(start + c * span, span)].astype(f32).reshape(rows, width)

        for c in range(chunks):
            normed = dot(to_pos, layer_norm(taken(x_ref, c), gain)).astype(bf16)
            for weight, held in ((wq_ref, q_ref), (wk_ref, k_ref), (wv_ref, v_ref)):
                product = dot(normed, weight[...]).astype(bf16).astype(f32)
                for p in range(owned):
                    held[p, c * span : (c + 1) * span, :] = product[p * span : (p + 1) * span]

        live = (key_at >= low) & (key_at < high)
        for p in range(owned):
            query, keys, values = q_ref[p], k_ref[p], v_ref[p]
            query = jnp.concatenate([jnp.where(keep, query, 0.0) for keep in in_down], 0)
            keys = jnp.concatenate([jnp.where(keep, keys, 0.0) for keep in in_across], 0)
            values = jnp.concatenate([jnp.where(keep, values, 0.0) for keep in in_across], 0)
            scores = dot_t(query.astype(bf16), keys.astype(bf16)) * scale
            scores = jnp.where(live, scores, masked_value)
            parts = []
            step = max(LANES, window)
            for at in range(0, across * window, step):
                part = scores[:, at : at + step]
                if window >= step:
                    top = jnp.max(part, axis=-1, keepdims=True)
                else:
                    group = iota(part.shape, 1) // window
                    top = jnp.zeros_like(part)
                    for g in range(step // window):
                        best = jnp.max(
                            jnp.where(group == g, part, masked_value), axis=-1, keepdims=True
                        )
                        top = jnp.where(group == g, best, top)
                parts.append(jnp.exp2(part - top).astype(bf16))
            exponent = jnp.concatenate(parts, 1)
            total = dot(exponent, ones)
            context = dot(exponent, values.astype(bf16)) / total
            joined = context[:window]
            for j in range(1, down):
                joined = jnp.where(in_down[j], context[j * window : (j + 1) * window], joined)
            c_ref[p] = joined

        for c in range(chunks):
            context = jnp.concatenate(
                [c_ref[p, c * span : (c + 1) * span, :] for p in range(owned)], 0
            ).astype(bf16)
            context = dot(to_slot, context).astype(bf16)
            middle = taken(x_ref, c) + dot(context, wo_ref[...])
            at = slot_at + c * span
            middle = jnp.where((at >= low) & (at < high), middle, taken(out_ref, c))
            out_ref[pl.ds(start + c * span, span)] = middle.reshape(span, owned, width).astype(bf16)
        return carry

    lax.fori_loop(0, mixtures, mixture, 0)


def attention(gathered, gain, w_query, w_key, w_value, w_out, counts, offsets):
    slots, owned, width = gathered.shape
    window = slots // counts.shape[0]
    vmem = pl.BlockSpec(memory_space=pltpu.VMEM)
    smem = pl.BlockSpec(memory_space=pltpu.SMEM)
    held = pltpu.VMEM((owned, window, width), f32)
    return pl.pallas_call(
        functools.partial(attention_kernel, window),
        out_shape=jax.ShapeDtypeStruct(gathered.shape, bf16),
        in_specs=[smem, smem] + [vmem] * 6,
        out_specs=vmem,
        scratch_shapes=[held] * 4,
        compiler_params=pltpu.CompilerParams(vmem_limit_bytes=48 * 1024 * 1024),
        cost_estimate=pl.CostEstimate(
            flops=14 * 10**9, bytes_accessed=2 * gathered.size * 2, transcendentals=10**6
        ),
        name="attention",
    )(counts, offsets, gathered, gain, w_query, w_key, w_value, w_out)


def feed_forward_kernel(each, x_ref, gain_ref, up_ref, down_ref, out_ref):
    width = x_ref.shape[-1]
    gain = gain_ref[...]
    for s in range(out_ref.shape[0]):
        middle = x_ref[:, s * each : (s + 1) * each, :].astype(f32).reshape(-1, width)
        second = layer_norm(middle, gain)
        hidden = jnp.maximum(dot(second, up_ref[...]), 0.0).astype(bf16)
        out_ref[s] = (middle + dot(hidden, down_ref[...])).astype(bf16)


def feed_forward(middle, groups, gain, w_up, w_down):
    devices, rows, width = middle.shape
    each = rows // groups
    if each % 8:
        middle = middle.reshape(devices, groups, each, width).swapaxes(0, 1)
        middle = middle.reshape(1, groups * devices * each, width)
        devices, each = 1, devices * each
    block = 4 if groups % 4 == 0 else 1
    whole = lambda shape: pl.BlockSpec(shape, lambda s: (0,) * len(shape))
    return pl.pallas_call(
        functools.partial(feed_forward_kernel, each),
        out_shape=jax.ShapeDtypeStruct((groups, devices * each, width), bf16),
        grid=(groups // block,),
        in_specs=[
            pl.BlockSpec((devices, block * each, width), lambda s: (0, s, 0)),
            whole(gain.shape),
            whole(w_up.shape),
            whole(w_down.shape),
        ],
        out_specs=pl.BlockSpec((block, devices * each, width), lambda s: (s, 0, 0)),
        compiler_params=pltpu.CompilerParams(vmem_limit_bytes=48 * 1024 * 1024),
        cost_estimate=pl.CostEstimate(
            flops=4 * middle.size * w_up.shape[1], bytes_accessed=4 * middle.size, transcendentals=0
        ),
        name="feed_forward",
    )(middle, gain, w_up, w_down)


def local(
    features, gain_attn, w_query, w_key, w_value, w_out, gain_ffn, w_up, w_down, counts, offsets
):
    axes = ("group", "pos")
    devices = lax.axis_size("group") * lax.axis_size("pos")
    groups, positions, width = features.shape
    owned = positions // devices
    slots = groups * devices
    sent = features.reshape(groups, devices, owned, width).swapaxes(0, 1)
    sent = sent.reshape(slots, owned, width)
    gathered = lax.all_to_all(sent, axes, split_axis=0, concat_axis=0, tiled=True)
    middle = attention(
        gathered, gain_attn.reshape(1, width), w_query, w_key, w_value, w_out, counts, offsets
    )
    returned = lax.all_to_all(middle, axes, split_axis=0, concat_axis=0, tiled=True)
    returned = returned.reshape(devices, groups * owned, width)
    return feed_forward(returned, groups, gain_ffn.reshape(1, width), w_up, w_down)


def solution(mesh):
    return jax.shard_map(
        local,
        mesh=mesh,
        in_specs=(P(("group", "pos"), None, None),) + (P(),) * 10,
        out_specs=P(("group", "pos"), None, None),
        check_vma=False,
    )
```

```python
import functools
import math

import jax
import jax.numpy as jnp
from jax import lax
from jax.experimental import pallas as pl
from jax.experimental.pallas import tpu as pltpu
from jax.sharding import PartitionSpec as P

HEADS = 8
LANES = 128


epsilon = 1e-05
masked_value = -1e30
f32 = jnp.float32
bf16 = jnp.bfloat16


def layer_norm(floats, gain):
    average = jnp.mean(floats, axis=-1, keepdims=True)
    centred = floats - average
    spread = jnp.mean(centred * centred, axis=-1, keepdims=True)
    return (centred * lax.rsqrt(spread + epsilon) * gain).astype(bf16)


def dot(a, b):
    return lax.dot_general(a, b, (((1,), (0,)), ((), ())), preferred_element_type=f32)


def dot_t(a, b):
    return lax.dot_general(a, b, (((1,), (1,)), ((), ())), preferred_element_type=f32)


def iota(shape, dim):
    return lax.broadcasted_iota(jnp.int32, shape, dim)


def attention_kernel(
    window,
    counts_ref,
    offsets_ref,
    x_ref,
    gain_ref,
    wq_ref,
    wk_ref,
    wv_ref,
    wo_ref,
    out_ref,
    *held,
):
    slots, owned, width = x_ref.shape
    head_dim = width // HEADS
    mixtures = counts_ref.shape[0]
    span = min(window, max(1, 256 // owned))
    rows = span * owned
    chunks = window // span
    scale = math.log2(math.e) / math.sqrt(head_dim)
    across = max(1, min(HEADS, width // window))
    down = HEADS // across
    row, col = iota((rows, rows), 0), iota((rows, rows), 1)
    to_pos = ((row % span) * owned + row // span == col).astype(f32).astype(bf16)
    to_slot = ((col % span) * owned + col // span == row).astype(f32).astype(bf16)
    gain = gain_ref[...]
    lane = iota((window, width), 1) // head_dim
    in_down = [lane % down == j for j in range(down)]
    in_across = [lane // down == i for i in range(across)]
    slot_at = iota((rows, width), 0) // owned
    pooled = (across * window, width)
    ones = iota(pooled, 0) // window == iota(pooled, 1) // (head_dim * down)
    ones = ones.astype(f32).astype(bf16)
    none = jnp.zeros((window, width), bf16)
    out_ref[...] = x_ref[...]

    def place(m):
        m = jnp.clip(m, 0, mixtures - 1)
        begin = offsets_ref[m]
        start = jnp.minimum(begin, slots - window)
        return start, begin - start, begin - start + counts_ref[m]

    def taken(ref, start, c):
        return ref[pl.ds(start + c * span, span)].astype(f32).reshape(rows, width)

    def project(m, q_ref, k_ref, v_ref, c_ref):
        start, _, _ = place(m)
        for c in range(chunks):
            normed = dot(to_pos, layer_norm(taken(x_ref, start, c), gain)).astype(bf16)
            for weight, held in ((wq_ref, q_ref), (wk_ref, k_ref), (wv_ref, v_ref)):
                product = dot(normed, weight[...])
                if held is q_ref:
                    product = product * scale
                product = product.astype(bf16)
                for p in range(owned):
                    held[p, c * span : (c + 1) * span, :] = product[p * span : (p + 1) * span]

    def stacked(values, masks):
        return jnp.concatenate([jnp.where(mask, values, none) for mask in masks], 0)

    def join(parts):
        joined = parts[:window]
        for j in range(1, down):
            joined = jnp.where(in_down[j], parts[j * window : (j + 1) * window], joined)
        return joined

    def attend(m, q_ref, k_ref, v_ref, c_ref):
        _, low, high = place(m)
        step = max(LANES, window)
        key_at = iota((down * window, step), 1)
        group = key_at // window
        live = (key_at % window >= low) & (key_at % window < high)
        masks = [live & (group == g) for g in range(step // window)]
        for p in range(owned):
            scores = dot_t(stacked(q_ref[p], in_down), stacked(k_ref[p], in_across))
            parts = []
            for at in range(0, across * window, step):
                part = scores[:, at : at + step]
                top = None
                for g, mask in enumerate(masks):
                    best = jnp.max(jnp.where(mask, part, masked_value), axis=-1, keepdims=True)
                    top = best if top is None else jnp.where(group == g, best, top)
                parts.append(jnp.exp2(jnp.where(live, part - top, masked_value)).astype(bf16))
            exponent = jnp.concatenate(parts, 1)
            total = join(dot(exponent, ones))
            c_ref[p] = join(dot(exponent, stacked(v_ref[p], in_across))) / total

    def finish(m, q_ref, k_ref, v_ref, c_ref):
        start, low, high = place(m)
        high = jnp.where(m < 0, low, high)
        for c in range(chunks):
            context = jnp.concatenate(
                [c_ref[p, c * span : (c + 1) * span, :] for p in range(owned)], 0
            ).astype(bf16)
            context = dot(to_slot, context).astype(bf16)
            middle = taken(x_ref, start, c) + dot(context, wo_ref[...])
            at = slot_at + c * span
            middle = jnp.where((at >= low) & (at < high), middle, taken(out_ref, start, c))
            out_ref[pl.ds(start + c * span, span)] = middle.reshape(span, owned, width).astype(bf16)

    even, odd = held[:4], held[4:]
    odd[3][...] = jnp.zeros(odd[3].shape, f32)
    project(0, *even)

    def pair(i, carry):
        m = 2 * i
        for now, this, other in ((m, even, odd), (m + 1, odd, even)):
            finish(now - 1, *other)
            attend(now, *this)
            project(now + 1, *other)
        return carry

    lax.fori_loop(0, pl.cdiv(mixtures, 2), pair, 0)
    finish(2 * pl.cdiv(mixtures, 2) - 1, *odd)


def attention(gathered, gain, w_query, w_key, w_value, w_out, counts, offsets):
    slots, owned, width = gathered.shape
    window = slots // counts.shape[0]
    vmem = pl.BlockSpec(memory_space=pltpu.VMEM)
    smem = pl.BlockSpec(memory_space=pltpu.SMEM)
    held = pltpu.VMEM((owned, window, width), bf16)
    return pl.pallas_call(
        functools.partial(attention_kernel, window),
        out_shape=jax.ShapeDtypeStruct(gathered.shape, bf16),
        in_specs=[smem, smem] + [vmem] * 6,
        out_specs=vmem,
        scratch_shapes=([held] * 3 + [pltpu.VMEM((owned, window, width), f32)]) * 2,
        compiler_params=pltpu.CompilerParams(vmem_limit_bytes=48 * 1024 * 1024),
        cost_estimate=pl.CostEstimate(
            flops=14 * 10**9, bytes_accessed=2 * gathered.size * 2, transcendentals=10**6
        ),
        name="attention",
    )(counts, offsets, gathered, gain, w_query, w_key, w_value, w_out)


def feed_forward_kernel(each, x_ref, gain_ref, up_ref, down_ref, out_ref):
    width = x_ref.shape[-1]
    gain = gain_ref[...]
    for s in range(out_ref.shape[0]):
        middle = x_ref[:, s * each : (s + 1) * each, :].astype(f32).reshape(-1, width)
        second = layer_norm(middle, gain)
        hidden = jnp.maximum(dot(second, up_ref[...]), 0.0).astype(bf16)
        out_ref[s] = (middle + dot(hidden, down_ref[...])).astype(bf16)


def feed_forward(middle, groups, gain, w_up, w_down):
    devices, rows, width = middle.shape
    each = rows // groups
    if each % 8:
        middle = middle.reshape(devices, groups, each, width).swapaxes(0, 1)
        middle = middle.reshape(1, groups * devices * each, width)
        devices, each = 1, devices * each
    block = 4 if groups % 4 == 0 else 1
    whole = lambda shape: pl.BlockSpec(shape, lambda s: (0,) * len(shape))
    return pl.pallas_call(
        functools.partial(feed_forward_kernel, each),
        out_shape=jax.ShapeDtypeStruct((groups, devices * each, width), bf16),
        grid=(groups // block,),
        in_specs=[
            pl.BlockSpec((devices, block * each, width), lambda s: (0, s, 0)),
            whole(gain.shape),
            whole(w_up.shape),
            whole(w_down.shape),
        ],
        out_specs=pl.BlockSpec((block, devices * each, width), lambda s: (s, 0, 0)),
        compiler_params=pltpu.CompilerParams(vmem_limit_bytes=48 * 1024 * 1024),
        cost_estimate=pl.CostEstimate(
            flops=4 * middle.size * w_up.shape[1], bytes_accessed=4 * middle.size, transcendentals=0
        ),
        name="feed_forward",
    )(middle, gain, w_up, w_down)


def local(
    features, gain_attn, w_query, w_key, w_value, w_out, gain_ffn, w_up, w_down, counts, offsets
):
    axes = ("group", "pos")
    devices = lax.axis_size("group") * lax.axis_size("pos")
    groups, positions, width = features.shape
    owned = positions // devices
    slots = groups * devices
    sent = features.reshape(groups, devices, owned, width).swapaxes(0, 1)
    sent = sent.reshape(slots, owned, width)
    gathered = lax.all_to_all(sent, axes, split_axis=0, concat_axis=0, tiled=True)
    middle = attention(
        gathered, gain_attn.reshape(1, width), w_query, w_key, w_value, w_out, counts, offsets
    )
    returned = lax.all_to_all(middle, axes, split_axis=0, concat_axis=0, tiled=True)
    returned = returned.reshape(devices, groups * owned, width)
    return feed_forward(returned, groups, gain_ffn.reshape(1, width), w_up, w_down)


def solution(mesh):
    return jax.shard_map(
        local,
        mesh=mesh,
        in_specs=(P(("group", "pos"), None, None),) + (P(),) * 10,
        out_specs=P(("group", "pos"), None, None),
        check_vma=False,
    )
```

```python
import functools
import math

import jax
import jax.numpy as jnp
from jax import lax
from jax.experimental import pallas as pl
from jax.experimental.pallas import tpu as pltpu
from jax.sharding import PartitionSpec as P

HEADS = 8
LANES = 128


epsilon = 1e-05
masked_value = -1e30
f32 = jnp.float32
bf16 = jnp.bfloat16


def layer_norm(floats, gain):
    average = jnp.mean(floats, axis=-1, keepdims=True)
    centred = floats - average
    spread = jnp.mean(centred * centred, axis=-1, keepdims=True)
    return (centred * lax.rsqrt(spread + epsilon) * gain).astype(bf16)


def dot(a, b):
    return lax.dot_general(a, b, (((1,), (0,)), ((), ())), preferred_element_type=f32)


def dot_t(a, b):
    return lax.dot_general(a, b, (((1,), (1,)), ((), ())), preferred_element_type=f32)


def iota(shape, dim):
    return lax.broadcasted_iota(jnp.int32, shape, dim)


def attention_kernel(
    window,
    counts_ref,
    offsets_ref,
    x_ref,
    gain_ref,
    wq_ref,
    wk_ref,
    wv_ref,
    wo_ref,
    out_ref,
    *held,
):
    slots, owned, width = x_ref.shape
    head_dim = width // HEADS
    mixtures = counts_ref.shape[0]
    span = min(window, max(1, 256 // owned))
    rows = span * owned
    chunks = window // span
    scale = math.log2(math.e) / math.sqrt(head_dim)
    across = max(1, min(HEADS, width // window))
    down = HEADS // across
    row, col = iota((rows, rows), 0), iota((rows, rows), 1)
    to_pos = ((row % span) * owned + row // span == col).astype(f32).astype(bf16)
    to_slot = ((col % span) * owned + col // span == row).astype(f32).astype(bf16)
    gain = gain_ref[...]
    lane = iota((window, width), 1) // head_dim
    in_down = [lane % down == j for j in range(down)]
    in_across = [lane // down == i for i in range(across)]
    slot_at = iota((rows, width), 0) // owned
    pooled = (across * window, width)
    ones = iota(pooled, 0) // window == iota(pooled, 1) // (head_dim * down)
    ones = ones.astype(f32).astype(bf16)
    none = jnp.zeros((window, width), bf16)
    out_ref[...] = x_ref[...]

    def place(m):
        begin = offsets_ref[m]
        start = jnp.minimum(begin, slots - window)
        return start, begin - start, begin - start + counts_ref[m]

    def taken(ref, start, c):
        return ref[pl.ds(start + c * span, span)].astype(f32).reshape(rows, width)

    def project(m, q_ref, k_ref, v_ref, c_ref):
        start, _, _ = place(m)
        for c in range(chunks):
            normed = dot(to_pos, layer_norm(taken(x_ref, start, c), gain)).astype(bf16)
            for weight, held in ((wq_ref, q_ref), (wk_ref, k_ref), (wv_ref, v_ref)):
                product = dot(normed, weight[...])
                if held is q_ref:
                    product = product * scale
                product = product.astype(bf16)
                for p in range(owned):
                    held[p, c * span : (c + 1) * span, :] = product[p * span : (p + 1) * span]

    def stacked(values, masks):
        return jnp.concatenate([jnp.where(mask, values, none) for mask in masks], 0)

    def join(parts):
        joined = parts[:window]
        for j in range(1, down):
            joined = jnp.where(in_down[j], parts[j * window : (j + 1) * window], joined)
        return joined

    def attend(m, q_ref, k_ref, v_ref, c_ref):
        _, low, high = place(m)
        step = max(LANES, window)
        key_at = iota((down * window, step), 1)
        group = key_at // window
        live = (key_at % window >= low) & (key_at % window < high)
        masks = [live & (group == g) for g in range(step // window)]
        for p in range(owned):
            scores = dot_t(stacked(q_ref[p], in_down), stacked(k_ref[p], in_across))
            parts = []
            for at in range(0, across * window, step):
                part = scores[:, at : at + step]
                top = None
                for g, mask in enumerate(masks):
                    best = jnp.max(jnp.where(mask, part, masked_value), axis=-1, keepdims=True)
                    top = best if top is None else jnp.where(group == g, best, top)
                parts.append(jnp.exp2(jnp.where(live, part - top, masked_value)).astype(bf16))
            exponent = jnp.concatenate(parts, 1)
            total = join(dot(exponent, ones))
            c_ref[p] = join(dot(exponent, stacked(v_ref[p], in_across))) / total

    def finish(m, q_ref, k_ref, v_ref, c_ref):
        start, low, high = place(m)
        for c in range(chunks):
            context = jnp.concatenate(
                [c_ref[p, c * span : (c + 1) * span, :] for p in range(owned)], 0
            ).astype(bf16)
            context = dot(to_slot, context).astype(bf16)
            middle = taken(x_ref, start, c) + dot(context, wo_ref[...])
            at = slot_at + c * span
            middle = jnp.where((at >= low) & (at < high), middle, taken(out_ref, start, c))
            out_ref[pl.ds(start + c * span, span)] = middle.reshape(span, owned, width).astype(bf16)

    even, odd = held[:4], held[4:]
    project(0, *even)

    for m in range(mixtures):
        this, other = (odd, even) if m % 2 else (even, odd)
        if m > 0:
            finish(m - 1, *other)
        attend(m, *this)
        if m + 1 < mixtures:
            project(m + 1, *other)
    finish(mixtures - 1, *this)


def attention(gathered, gain, w_query, w_key, w_value, w_out, counts, offsets):
    slots, owned, width = gathered.shape
    window = slots // counts.shape[0]
    vmem = pl.BlockSpec(memory_space=pltpu.VMEM)
    smem = pl.BlockSpec(memory_space=pltpu.SMEM)
    held = pltpu.VMEM((owned, window, width), bf16)
    return pl.pallas_call(
        functools.partial(attention_kernel, window),
        out_shape=jax.ShapeDtypeStruct(gathered.shape, bf16),
        in_specs=[smem, smem] + [vmem] * 6,
        out_specs=vmem,
        scratch_shapes=([held] * 3 + [pltpu.VMEM((owned, window, width), f32)]) * 2,
        compiler_params=pltpu.CompilerParams(vmem_limit_bytes=48 * 1024 * 1024),
        cost_estimate=pl.CostEstimate(
            flops=14 * 10**9, bytes_accessed=2 * gathered.size * 2, transcendentals=10**6
        ),
        name="attention",
    )(counts, offsets, gathered, gain, w_query, w_key, w_value, w_out)


def feed_forward_kernel(each, x_ref, gain_ref, up_ref, down_ref, out_ref, held_ref, sems):
    width = x_ref.shape[-1]
    groups = held_ref.shape[0]
    gain = gain_ref[...]

    def leave(s):
        return pltpu.make_async_copy(held_ref.at[s], out_ref.at[s], sems.at[s])

    for s in range(groups):
        middle = x_ref[:, s * each : (s + 1) * each, :].astype(f32).reshape(-1, width)
        second = layer_norm(middle, gain)
        hidden = jnp.maximum(dot(second, up_ref[...]), 0.0).astype(bf16)
        held_ref[s] = (middle + dot(hidden, down_ref[...])).astype(bf16)
        leave(s).start()
    for s in range(groups):
        leave(s).wait()


def feed_forward(middle, groups, gain, w_up, w_down):
    devices, rows, width = middle.shape
    each = rows // groups
    if each % 8:
        middle = middle.reshape(devices, groups, each, width).swapaxes(0, 1)
        middle = middle.reshape(1, groups * devices * each, width)
        devices, each = 1, devices * each
    vmem = pl.BlockSpec(memory_space=pltpu.VMEM)
    shape = (groups, devices * each, width)
    return pl.pallas_call(
        functools.partial(feed_forward_kernel, each),
        out_shape=jax.ShapeDtypeStruct(shape, bf16),
        in_specs=[vmem] * 4,
        out_specs=pl.BlockSpec(memory_space=pl.ANY),
        scratch_shapes=[pltpu.VMEM(shape, bf16), pltpu.SemaphoreType.DMA((groups,))],
        compiler_params=pltpu.CompilerParams(vmem_limit_bytes=48 * 1024 * 1024),
        cost_estimate=pl.CostEstimate(
            flops=4 * middle.size * w_up.shape[1], bytes_accessed=4 * middle.size, transcendentals=0
        ),
        name="feed_forward",
    )(middle, gain, w_up, w_down)


def local(
    features, gain_attn, w_query, w_key, w_value, w_out, gain_ffn, w_up, w_down, counts, offsets
):
    axes = ("group", "pos")
    devices = lax.axis_size("group") * lax.axis_size("pos")
    groups, positions, width = features.shape
    owned = positions // devices
    slots = groups * devices
    sent = features.reshape(groups, devices, owned, width).swapaxes(0, 1)
    sent = sent.reshape(slots, owned, width)
    gathered = lax.all_to_all(sent, axes, split_axis=0, concat_axis=0, tiled=True)
    middle = attention(
        gathered, gain_attn.reshape(1, width), w_query, w_key, w_value, w_out, counts, offsets
    )
    returned = lax.all_to_all(middle, axes, split_axis=0, concat_axis=0, tiled=True)
    returned = returned.reshape(devices, groups * owned, width)
    return feed_forward(returned, groups, gain_ffn.reshape(1, width), w_up, w_down)


def solution(mesh):
    return jax.shard_map(
        local,
        mesh=mesh,
        in_specs=(P(("group", "pos"), None, None),) + (P(),) * 10,
        out_specs=P(("group", "pos"), None, None),
        check_vma=False,
    )
```
